32 devices in a mesh: band: 8 (over z, y), feat: 4 (over x, core).
Axes of the slice: x: 2, y: 2, z: 4, core: 2. Of those that a mesh axis runs over, the one named last changes fastest.
Arguments:
- grid_latent: bfloat16 [16384, 512], P('band', 'feat'), may hold values from -6 to 6
- mesh_latent: bfloat16 [1280, 512], P('band', 'feat'), may hold values from -6 to 6
- edge_latent: bfloat16 [8, 4, 2048, 512], P('band', 'feat'), may hold values from -6 to 6
- edge_src: int32 [8, 8192], P('band'), may hold values from 0 to 2047
- edge_dst: int32 [8, 4, 2048], P('band', 'feat'), may hold values from 0 to 160, as said below
- edge_w1: bfloat16 [1536, 512], replicated, may hold values from -0.15625 to 0.15625
- edge_b1: float32 [512], replicated, may hold values from -3 to 3
- edge_w2: bfloat16 [512, 512], replicated, may hold values from -0.25 to 0.25
- edge_b2: float32 [512], replicated, may hold values from -2 to 2
- edge_gain: float32 [512], replicated, may hold values from 0.25 to 1.75
- edge_shift: float32 [512], replicated, may hold values from -2 to 2
- node_w1: bfloat16 [1024, 512], replicated, may hold values from -0.1875 to 0.1875
- node_b1: float32 [512], replicated, may hold values from -3 to 3
- node_w2: bfloat16 [512, 512], replicated, may hold values from -0.25 to 0.25
- node_b2: float32 [512], replicated, may hold values from -2 to 2
- node_gain: float32 [512], replicated, may hold values from 0.25 to 1.75
- node_shift: float32 [512], replicated, may hold values from -2 to 2
Outputs:
- mesh_new: bfloat16 [1280, 512], P('band', 'feat')
The draws below stay inside these ranges and needn't reach their ends.
Inputs may be any that keep to these rules, and one draw needn't show every extreme that they name: `edge_src`: entry [s, d * 1024 + j] is the grid row, counted within band index s, that sends slot j of the edges from band index s to band index d; empty slots hold some row too. `edge_dst`: entry [d, f, s * 256 + q] is the mesh node, counted within band index d, that receives slot f * 256 + q of the edges from band index s to band index d, or 160 where that slot is empty. The used slots of a pair come first; a pair has at most 1024 used slots. Each receiving band index d hears only from the sending band indices of one latitude span of consecutive indices (edges are local), which lies anywhere along band since mesh partitions are face-major; other pairs are empty. In every draw some band indices receive 1024 from every band index of their span.
All inputs are finite; a program needn't handle non-finite values.
Results may differ from the reference program's by a relative error of at most 0.011.
Values may be sent and summed in bfloat16 or wider, within the bound.
A program may use at most 64 MiB of HBM per device.

```python
import jax
import jax.numpy as jnp
from jax import lax

D = 512
H = 512
G_DEV = 2048
M_DEV = 160
CAP = 1024
QUART = 256
GRID = 16384
MESH = 1280
N_BAND = 8
N_FEAT = 4


def pair_counts(key):
    base_key = jax.random.fold_in(key, 7)
    count_key, crowd_key, forced_key, center_key, half_key = jax.random.split(base_key, 5)
    counts = jax.random.randint(count_key, (N_BAND, N_BAND), 1, CAP + 1)
    crowded = jax.random.randint(crowd_key, (N_BAND,), 0, 8) == 0
    forced = jax.random.randint(forced_key, (), 0, N_BAND)
    crowded = crowded | (jnp.arange(N_BAND) == forced)
    centers = jax.random.randint(center_key, (N_BAND,), 0, N_BAND)
    halves = jax.random.randint(half_key, (N_BAND,), 3, 9)
    senders = jnp.arange(N_BAND)[:, None]
    linked = jnp.abs(senders - centers[None, :]) <= halves[None, :]
    counts = jnp.where(crowded[None, :], CAP, counts)
    return jnp.where(linked, counts, 0)


def draw_edge_dst(key, part):
    counts = pair_counts(key)
    node_key = jax.random.fold_in(key, 21)
    first_key, hot_key, pick_key, use_key = jax.random.split(node_key, 4)
    shape = (N_BAND, N_FEAT, N_BAND, QUART)
    uniform_node = jax.random.randint(first_key, shape, 0, M_DEV)
    hot_nodes = jax.random.randint(hot_key, (N_BAND, 4), 0, M_DEV)
    picks = jax.random.randint(pick_key, shape, 0, 4)
    use_hot = jax.random.randint(use_key, shape, 0, 3) == 0
    chosen = jnp.sum(jnp.where(picks[..., None] == jnp.arange(4), hot_nodes[:, None, None, None, :], 0), -1)
    nodes_all = jnp.where(use_hot, chosen, uniform_node)
    slot_index = jnp.arange(N_FEAT)[None, :, None, None] * QUART + jnp.arange(QUART)[None, None, None, :]
    filled = slot_index < jnp.transpose(counts)[:, None, :, None]
    result = jnp.where(filled, nodes_all, M_DEV)
    return result.reshape(N_BAND, N_FEAT, N_BAND * QUART).astype(jnp.int32)


def place_ends(drawn, stream_key, least, high):
    shape = drawn.shape
    index_at = [jax.random.randint(jax.random.fold_in(stream_key, axis), (), 0, shape[axis]) for axis in range(len(shape))]
    drawn = drawn.at[tuple(index_at)].set(least)
    longest = shape.index(max(shape))
    index_at[longest] = (index_at[longest] + 1) % shape[longest]
    return drawn.at[tuple(index_at)].set(high)


def steps_of(own_key, shape, cuts, low, largest):
    def one(axis_at, blocks):
        heights = jax.random.uniform(jax.random.fold_in(jax.random.fold_in(own_key, 6), axis_at), (blocks,), jnp.float32, low / len(cuts), largest / len(cuts))
        return jnp.repeat(jnp.exp(heights), shape[axis_at] // blocks).reshape((-1,) + (1,) * (len(shape) - axis_at - 1))

    gain = one(*cuts[0])
    for cut in cuts[1:]:
        gain = gain * one(*cut)
    return gain


def noise(own_key, extent, deviation, most, cuts=(), held_as=jnp.bfloat16):
    factor_of = steps_of(own_key, extent, cuts, -0.22, 0.18) if cuts else 1.0
    array = jax.random.normal(own_key, extent, jnp.float32) * deviation * factor_of
    return jnp.minimum(jnp.maximum(array, -most), most).astype(held_as)


def setup_inputs(seed: int = 0) -> dict:
    streams_of = jax.random.split(jax.random.key(seed), 18)
    grid_latent = noise(streams_of[0], (GRID, D), 1.0, 6.0, ((0, 8), (1, 4)))
    mesh_latent = noise(streams_of[1], (MESH, D), 1.0, 6.0, ((0, 8), (1, 4)))
    edge_latent = noise(streams_of[2], (N_BAND, N_FEAT, N_BAND * QUART, D), 1.0, 6.0, ((0, 8), (1, 4)))
    edge_src = place_ends(jax.random.randint(streams_of[3], (N_BAND, N_BAND * CAP), 0, G_DEV), jax.random.fold_in(streams_of[3], 1), 0, G_DEV - 1).astype(jnp.int32)
    edge_dst = draw_edge_dst(jax.random.fold_in(streams_of[17], 71), 0)
    edge_w1 = noise(streams_of[5], (3 * D, H), (3 * D) ** -0.5, 0.15625)
    edge_b1 = noise(streams_of[6], (H,), 0.5, 3.0, (), jnp.float32)
    edge_w2 = noise(streams_of[7], (H, D), H ** -0.5, 0.25)
    edge_b2 = noise(streams_of[8], (D,), 0.3, 2.0, (), jnp.float32)
    edge_gain = jnp.clip(1.0 + 0.15 * jax.random.normal(streams_of[9], (D,), jnp.float32), 0.25, 1.75)
    edge_shift = noise(streams_of[10], (D,), 0.3, 2.0, (), jnp.float32)
    node_w1 = noise(streams_of[11], (2 * D, H), (2 * D) ** -0.5, 0.1875)
    node_b1 = noise(streams_of[12], (H,), 0.5, 3.0, (), jnp.float32)
    node_w2 = noise(streams_of[13], (H, D), H ** -0.5, 0.25)
    node_b2 = noise(streams_of[14], (D,), 0.3, 2.0, (), jnp.float32)
    node_gain = jnp.clip(1.0 + 0.15 * jax.random.normal(streams_of[15], (D,), jnp.float32), 0.25, 1.75)
    node_shift = noise(streams_of[16], (D,), 0.3, 2.0, (), jnp.float32)
    return {"grid_latent": grid_latent, "mesh_latent": mesh_latent, "edge_latent": edge_latent, "edge_src": edge_src, "edge_dst": edge_dst, "edge_w1": edge_w1, "edge_b1": edge_b1, "edge_w2": edge_w2, "edge_b2": edge_b2, "edge_gain": edge_gain, "edge_shift": edge_shift, "node_w1": node_w1, "node_b1": node_b1, "node_w2": node_w2, "node_b2": node_b2, "node_gain": node_gain, "node_shift": node_shift}


EPSILON = 1e-05

def normalize(values, norm_gain, norm_shift):
    average = lax.optimization_barrier(jnp.mean(values, -1, keepdims=True))
    centered = values - average
    variance = lax.optimization_barrier(jnp.mean(centered * centered, -1, keepdims=True))
    return centered * lax.rsqrt(variance + EPSILON) * norm_gain + norm_shift

def reference(grid_latent, mesh_latent, edge_latent, edge_src, edge_dst, edge_w1, edge_b1, edge_w2, edge_b2, edge_gain, edge_shift, node_w1, node_b1, node_w2, node_b2, node_gain, node_shift):
    full_width = grid_latent.shape[1]
    slot_count = N_FEAT * N_BAND * QUART
    local_src = edge_src.reshape(N_BAND, N_BAND, N_FEAT, QUART)
    offsets = (jnp.arange(N_BAND, dtype=jnp.int32) * G_DEV)[:, None, None, None]
    global_src = jnp.transpose(local_src + offsets, (1, 2, 0, 3)).reshape(N_BAND, slot_count)

    def one_owner(owner):
        source_rows = global_src[owner]
        senders = jnp.take(grid_latent, source_rows, axis=0)
        own_edges = edge_latent[owner].reshape(slot_count, full_width)
        targets = edge_dst[owner].reshape(slot_count)
        mesh_rows = lax.dynamic_slice_in_dim(mesh_latent, (owner * M_DEV).astype(jnp.int32), M_DEV, 0)
        receivers = jnp.take(mesh_rows, jnp.clip(targets, 0, M_DEV - 1), axis=0)
        joined = jnp.concatenate([own_edges, senders, receivers], 1)
        hidden = jnp.dot(joined, edge_w1, preferred_element_type=jnp.float32) + edge_b1
        active = jax.nn.silu(hidden).astype(jnp.bfloat16)
        update = jnp.dot(active, edge_w2, preferred_element_type=jnp.float32) + edge_b2
        edge_new = (own_edges.astype(jnp.float32) + normalize(update, edge_gain, edge_shift)).astype(jnp.bfloat16)
        summed = jax.ops.segment_sum(edge_new.astype(jnp.float32), targets, num_segments=M_DEV + 1)[:M_DEV]
        node_in = jnp.concatenate([mesh_rows, summed.astype(jnp.bfloat16)], 1)
        node_hidden = jnp.dot(node_in, node_w1, preferred_element_type=jnp.float32) + node_b1
        node_active = jax.nn.silu(node_hidden).astype(jnp.bfloat16)
        node_update = jnp.dot(node_active, node_w2, preferred_element_type=jnp.float32) + node_b2
        return (mesh_rows.astype(jnp.float32) + normalize(node_update, node_gain, node_shift)).astype(jnp.bfloat16)
    updated = lax.map(one_owner, jnp.arange(N_BAND, dtype=jnp.int32))
    return updated.reshape(N_BAND * M_DEV, full_width)
```

```python
import functools

import jax
import jax.numpy as jnp
from jax import lax
from jax.experimental import pallas as pl
from jax.experimental.pallas import tpu as pltpu
from jax.sharding import PartitionSpec as P

EPSILON = 1e-05
LANES = 128
CHUNKS = 4
MESH = pl.DeviceIdType.MESH
F32 = jnp.float32
BF16 = jnp.bfloat16


def normalize(values, norm_gain, norm_shift):
    average = jnp.mean(values, -1, keepdims=True)
    centered = values - average
    variance = jnp.mean(centered * centered, -1, keepdims=True)
    return centered * lax.rsqrt(variance + EPSILON) * norm_gain + norm_shift


def silu(v):
    half = 0.5 * v
    return half + half * jnp.tanh(half)


def dot(a, b):
    return jnp.dot(a, b, preferred_element_type=F32)


def columns(row):
    return jnp.broadcast_to(row, (LANES, LANES)).T


def kernel(
    n,
    nf,
    grid_ref,
    mesh_ref,
    src_ref,
    dst_ref,
    dst_wide,
    vec_ref,
    edge_hbm,
    w1_hbm,
    w2_hbm,
    nw1_hbm,
    nw2_hbm,
    out_ref,
    edge,
    w1,
    w2,
    nw1,
    nw2,
    table,
    nodes,
    onehot,
    outgoing,
    arrived,
    base,
    mesh_full,
    total,
    parts,
    part_in,
    cols_out,
    cols_in,
    local_sem,
    mesh_send,
    mesh_recv,
    core_sem,
    x_send,
    x_recv,
    fwd_send,
    fwd_recv,
    band_send,
    band_recv,
    sum_send,
    sum_recv,
    out_send,
    out_recv,
):
    b = lax.axis_index("band")
    f = lax.axis_index("feat")
    grid_rows = grid_ref.shape[0]
    quarter = grid_ref.shape[1]
    width = quarter * nf
    slots = edge.shape[0]
    quart = slots // n
    mesh_rows = mesh_ref.shape[0]
    own_rows = mesh_rows // nf
    pair = 2 * quarter
    h = f // 2
    c = lax.rem(f, 2)
    core_peer = h * 2 + (1 - c)
    x_peer = (1 - h) * 2 + c

    loads = [
        pltpu.make_async_copy(a, v, local_sem.at[i])
        for i, (a, v) in enumerate(
            ((w1_hbm, w1), (edge_hbm, edge), (w2_hbm, w2), (nw1_hbm, nw1), (nw2_hbm, nw2))
        )
    ]
    for load in loads:
        load.start()

    barrier = pltpu.get_barrier_semaphore()
    for k in range(1, nf):
        pl.semaphore_signal(barrier, inc=1, device_id=(b, lax.rem(f + k, nf)), device_id_type=MESH)
    for k in range(1, n):
        pl.semaphore_signal(barrier, inc=1, device_id=(lax.rem(b + k, n), f), device_id_type=MESH)
    pl.semaphore_wait(barrier, nf - 1 + n - 1)

    def remote(src, dst, send, recv, band, feat):
        return pltpu.make_async_remote_copy(
            src_ref=src,
            dst_ref=dst,
            send_sem=send,
            recv_sem=recv,
            device_id=(band, feat),
            device_id_type=MESH,
        )

    def cols(i):
        return pl.ds(pl.multiple_of(i * quarter, quarter), quarter)

    step = grid_rows // CHUNKS

    def x_copy(i):
        rows = pl.ds(i * step, step)
        return remote(
            grid_ref.at[rows, :], table.at[h, rows, cols(c)], x_send.at[i], x_recv.at[i], b, x_peer
        )

    def fwd_copy(i):
        rows = pl.ds(i * step, step)
        place = table.at[1 - h, rows, cols(c)]
        return remote(place, place, fwd_send.at[i], fwd_recv.at[i], b, core_peer)

    core_copy = remote(
        grid_ref, table.at[h, :, cols(c)], core_sem.at[0], core_sem.at[1], b, core_peer
    )
    mesh_copies = [
        remote(mesh_ref, nodes.at[f], mesh_send.at[k - 1], mesh_recv.at[k - 1], b, lax.rem(f + k, nf))
        for k in range(1, nf)
    ]
    core_copy.start()
    x_copies = [x_copy(i) for i in range(CHUNKS)]
    for copy in x_copies:
        copy.start()
    for copy in mesh_copies:
        copy.start()

    nodes[f] = mesh_ref[...]
    table[h, :, cols(c)] = grid_ref[...]

    lane = lax.broadcasted_iota(jnp.int32, (LANES, LANES), 1)

    def build(t, carry):
        ids = columns(src_ref[pl.ds(t, 1), :])
        rows = pl.ds(pl.multiple_of(t * LANES, LANES), LANES)
        for k in range(grid_rows // LANES):
            hit = jnp.where(lane + k * LANES == ids, 1.0, 0.0)
            onehot[rows, k * LANES : (k + 1) * LANES] = hit.astype(BF16)
        return carry

    lax.fori_loop(0, slots // LANES, build, 0)
    core_copy.wait_recv()

    def band_copy(j, o):
        d = lax.rem(b + o, n)
        return remote(
            outgoing.at[j, o],
            arrived.at[j, b],
            band_send.at[j, o],
            band_recv.at[j, o],
            d,
            f,
        )

    def gather(j, half):
        def piece(o):
            d = lax.rem(b + o, n)
            rows = pl.ds(pl.multiple_of(d * quart, quart), quart)
            return dot(onehot[rows, :], table[half]).astype(BF16)

        def one(o, carry):
            outgoing[j, o] = piece(o)

            @pl.when(o > 1)
            def _():
                band_copy(j, o - 1).start()

            return carry

        lax.fori_loop(1, n, one, 0)
        arrived[j, b] = piece(0)
        band_copy(j, n - 1).start()

    gather(0, h)

    for load in loads[:2]:
        load.wait()
    for copy in mesh_copies:
        copy.wait_recv()
    mesh_wide = jnp.concatenate([nodes[k] for k in range(nf)], axis=1)
    mesh_full[...] = mesh_wide.astype(F32)
    block = 2 * LANES
    node_lane = lax.broadcasted_iota(jnp.int32, (LANES, mesh_rows), 1)
    b1 = vec_ref[0:1, :]

    def prepare(t, carry):
        picks = []
        for i in range(2):
            ids = columns(dst_wide[pl.ds(2 * t + i, 1), :])
            ids = jnp.minimum(ids, mesh_rows - 1)
            spread = jnp.concatenate([ids] * ((mesh_rows + LANES - 1) // LANES), axis=1)[:, :mesh_rows]
            hit = jnp.where(node_lane == spread, 1.0, 0.0).astype(BF16)
            picks.append(dot(hit, mesh_wide_ref()).astype(BF16))
        receivers = jnp.concatenate(picks, axis=0)
        rows = pl.ds(pl.multiple_of(t * block, block), block)
        base[rows, :] = (
            dot(edge[rows, :], w1[:width, :]) + dot(receivers, w1[2 * width :, :]) + b1
        )
        return carry

    def mesh_wide_ref():
        return jnp.concatenate([nodes[k] for k in range(nf)], axis=1)

    lax.fori_loop(0, slots // block, prepare, 0)
    for load in loads[2:]:
        load.wait()
    my_nodes = pl.ds(pl.multiple_of(f * own_rows, 8), own_rows)
    my_mesh = mesh_full[my_nodes, :]
    node_base = dot(my_mesh.astype(BF16), nw1[:width, :]) + vec_ref[4:5, :]

    fwd_copies = [fwd_copy(i) for i in range(CHUNKS)]
    for i in range(CHUNKS):
        x_copies[i].wait_recv()
        fwd_copies[i].start()
    for copy in fwd_copies:
        copy.wait_recv()
    gather(1, 1 - h)

    b2 = vec_ref[1:2, :]
    gain = vec_ref[2:3, :]
    shift = vec_ref[3:4, :]
    total[...] = jnp.zeros_like(total)
    node_row = lax.broadcasted_iota(jnp.int32, (mesh_rows, quart), 0)

    def edges(o, carry):
        s = lax.rem(b - o + n, n)

        @pl.when(o > 0)
        def _():
            band_copy(0, o).wait_recv()
            band_copy(1, o).wait_recv()

        rows = pl.ds(pl.multiple_of(s * quart, quart), quart)
        low = pl.ds(pl.multiple_of(width + h * pair, pair), pair)
        high = pl.ds(pl.multiple_of(width + (1 - h) * pair, pair), pair)
        hidden = base[rows, :] + dot(arrived[0, s], w1[low, :]) + dot(arrived[1, s], w1[high, :])
        update = dot(silu(hidden).astype(BF16), w2[...]) + b2
        fresh = (edge[rows, :].astype(F32) + normalize(update, gain, shift)).astype(BF16)
        hit = jnp.where(node_row == dst_ref[pl.ds(s, 1), :], 1.0, 0.0).astype(BF16)
        total[...] += dot(hit, fresh)
        return carry

    lax.fori_loop(0, n, edges, 0)

    for k in range(nf):
        parts[k] = total[k * own_rows : (k + 1) * own_rows, :].astype(BF16)
    sum_copies = []
    for k in range(1, nf):
        p = lax.rem(f + k, nf)
        sum_copies.append(
            remote(parts.at[p], part_in.at[k - 1], sum_send.at[k - 1], sum_recv.at[k - 1], b, p)
        )
    for copy in sum_copies:
        copy.start()
    summed = parts[f].astype(F32)
    for k in range(1, nf):
        sum_copies[k - 1].wait_recv()
        summed = summed + part_in[k - 1].astype(F32)
    hidden = node_base + dot(summed.astype(BF16), nw1[width:, :])
    update = dot(silu(hidden).astype(BF16), nw2[...]) + vec_ref[5:6, :]
    fresh = (my_mesh + normalize(update, vec_ref[6:7, :], vec_ref[7:8, :])).astype(BF16)
    for k in range(nf):
        cols_out[k] = fresh[:, k * quarter : (k + 1) * quarter]
    out_copies = []
    for k in range(1, nf):
        p = lax.rem(f + k, nf)
        out_copies.append(
            remote(cols_out.at[p], cols_in.at[f], out_send.at[k - 1], out_recv.at[k - 1], b, p)
        )
    for copy in out_copies:
        copy.start()
    cols_in[f] = cols_out[f]
    for copy in out_copies:
        copy.wait_recv()
    out_ref[...] = jnp.concatenate([cols_in[k].astype(F32) for k in range(nf)], axis=0).astype(BF16)

    core_copy.wait_send()
    for copy in x_copies + mesh_copies + fwd_copies + sum_copies + out_copies:
        copy.wait_send()

    def drain(o, carry):
        band_copy(0, o).wait_send()
        band_copy(1, o).wait_send()
        return carry

    lax.fori_loop(1, n, drain, 0)


def body(
    grid_latent,
    mesh_latent,
    edge_latent,
    edge_src,
    edge_dst,
    edge_w1,
    edge_b1,
    edge_w2,
    edge_b2,
    edge_gain,
    edge_shift,
    node_w1,
    node_b1,
    node_w2,
    node_b2,
    node_gain,
    node_shift,
):
    n = lax.axis_size("band")
    nf = lax.axis_size("feat")
    grid_rows, quarter = grid_latent.shape
    width = quarter * nf
    mesh_rows = mesh_latent.shape[0]
    own_rows = mesh_rows // nf
    edges = edge_latent.reshape(-1, width)
    slots = edges.shape[0]
    quart = slots // n
    hidden = edge_w1.shape[1]
    own_src = lax.dynamic_slice_in_dim(
        edge_src.reshape(n, nf, quart), lax.axis_index("feat"), 1, 1
    ).reshape(-1, LANES)
    vectors = jnp.stack(
        [edge_b1, edge_b2, edge_gain, edge_shift, node_b1, node_b2, node_gain, node_shift]
    )
    vmem = pl.BlockSpec(memory_space=pltpu.VMEM)
    anyspace = pl.BlockSpec(memory_space=pl.ANY)
    dma = pltpu.SemaphoreType.DMA
    return pl.pallas_call(
        functools.partial(kernel, n, nf),
        out_shape=jax.ShapeDtypeStruct((mesh_rows, quarter), BF16),
        in_specs=[vmem] * 6 + [anyspace] * 5,
        out_specs=vmem,
        scratch_shapes=[
            pltpu.VMEM((slots, width), BF16),
            pltpu.VMEM(edge_w1.shape, BF16),
            pltpu.VMEM(edge_w2.shape, BF16),
            pltpu.VMEM(node_w1.shape, BF16),
            pltpu.VMEM(node_w2.shape, BF16),
            pltpu.VMEM((nf // 2, grid_rows, 2 * quarter), BF16),
            pltpu.VMEM((nf, mesh_rows, quarter), BF16),
            pltpu.VMEM((slots, grid_rows), BF16),
            pltpu.VMEM((2, n, quart, 2 * quarter), BF16),
            pltpu.VMEM((2, n, quart, 2 * quarter), BF16),
            pltpu.VMEM((slots, hidden), F32),
            pltpu.VMEM((mesh_rows, width), F32),
            pltpu.VMEM((mesh_rows, width), F32),
            pltpu.VMEM((nf, own_rows, width), BF16),
            pltpu.VMEM((nf - 1, own_rows, width), BF16),
            pltpu.VMEM((nf, own_rows, quarter), BF16),
            pltpu.VMEM((nf, own_rows, quarter), BF16),
            dma((5,)),
            dma((nf - 1,)),
            dma((nf - 1,)),
            dma((2,)),
            dma((CHUNKS,)),
            dma((CHUNKS,)),
            dma((CHUNKS,)),
            dma((CHUNKS,)),
            dma((2, n)),
            dma((2, n)),
            dma((nf - 1,)),
            dma((nf - 1,)),
            dma((nf - 1,)),
            dma((nf - 1,)),
        ],
        compiler_params=pltpu.CompilerParams(
            collective_id=0, has_side_effects=True, vmem_limit_bytes=56 * 1024 * 1024
        ),
        name="encoder_step",
    )(
        grid_latent,
        mesh_latent,
        own_src,
        edge_dst.reshape(n, quart),
        edge_dst.reshape(-1, LANES),
        vectors,
        edges,
        edge_w1,
        edge_w2,
        node_w1,
        node_w2,
    )


def solution(mesh):
    placed = (
        P("band", "feat"),
        P("band", "feat"),
        P("band", "feat", None, None),
        P("band", None),
        P("band", "feat", None),
    ) + (P(),) * 12
    return jax.shard_map(
        body, mesh=mesh, in_specs=placed, out_specs=P("band", "feat"), check_vma=False
    )
```

```python
import functools

import jax
import jax.numpy as jnp
from jax import lax
from jax.experimental import pallas as pl
from jax.experimental.pallas import tpu as pltpu
from jax.sharding import PartitionSpec as P

EPSILON = 1e-05
LANES = 128
CHUNKS = 4
MESH = pl.DeviceIdType.MESH
F32 = jnp.float32
BF16 = jnp.bfloat16


def normalize(values, norm_gain, norm_shift):
    average = jnp.mean(values, -1, keepdims=True)
    centered = values - average
    variance = jnp.mean(centered * centered, -1, keepdims=True)
    return centered * lax.rsqrt(variance + EPSILON) * norm_gain + norm_shift


def silu(v):
    half = 0.5 * v
    return half + half * jnp.tanh(half)


def dot(a, b):
    return jnp.dot(a, b, preferred_element_type=F32)


def columns(row):
    return jnp.broadcast_to(row, (LANES, LANES)).T


def kernel(
    n,
    nf,
    grid_ref,
    mesh_ref,
    src_ref,
    dst_ref,
    dst_wide,
    b1_ref,
    b2_ref,
    gain_ref,
    shift_ref,
    nb1_ref,
    nb2_ref,
    ngain_ref,
    nshift_ref,
    edge_hbm,
    w1_hbm,
    w2_hbm,
    nw1_hbm,
    nw2_hbm,
    out_ref,
    edge,
    w1,
    w2,
    nw1,
    nw2,
    table,
    nodes,
    onehot,
    outgoing,
    arrived,
    base,
    mesh_full,
    total,
    parts,
    part_in,
    cols_out,
    cols_in,
    local_sem,
    mesh_send,
    mesh_recv,
    core_sem,
    x_send,
    x_recv,
    fwd_send,
    fwd_recv,
    band_send,
    band_recv,
    sum_send,
    sum_recv,
    out_send,
    out_recv,
):
    b = lax.axis_index("band")
    f = lax.axis_index("feat")
    grid_rows = grid_ref.shape[0]
    quarter = grid_ref.shape[1]
    width = quarter * nf
    slots = edge.shape[0]
    quart = slots // n
    aligned = quart % LANES == 0
    mesh_rows = mesh_ref.shape[0]
    own_rows = mesh_rows // nf
    pair = 2 * quarter
    h = f // 2
    c = lax.rem(f, 2)
    core_peer = h * 2 + (1 - c)
    x_peer = (1 - h) * 2 + c

    loads = [
        pltpu.make_async_copy(a, v, local_sem.at[i])
        for i, (a, v) in enumerate(
            ((w1_hbm, w1), (edge_hbm, edge), (w2_hbm, w2), (nw1_hbm, nw1), (nw2_hbm, nw2))
        )
    ]
    for load in loads:
        load.start()

    barrier = pltpu.get_barrier_semaphore()
    for k in range(1, nf):
        pl.semaphore_signal(barrier, inc=1, device_id=(b, lax.rem(f + k, nf)), device_id_type=MESH)
    for k in range(1, n):
        pl.semaphore_signal(barrier, inc=1, device_id=(lax.rem(b + k, n), f), device_id_type=MESH)
    pl.semaphore_wait(barrier, nf - 1 + n - 1)

    def remote(src, dst, send, recv, band, feat):
        return pltpu.make_async_remote_copy(
            src_ref=src,
            dst_ref=dst,
            send_sem=send,
            recv_sem=recv,
            device_id=(band, feat),
            device_id_type=MESH,
        )

    def cols(i):
        return pl.ds(pl.multiple_of(i * quarter, quarter), quarter)

    step = grid_rows // CHUNKS

    def x_copy(i):
        rows = pl.ds(i * step, step)
        return remote(
            grid_ref.at[rows, :], table.at[h, rows, cols(c)], x_send.at[i], x_recv.at[i], b, x_peer
        )

    def fwd_copy(i):
        rows = pl.ds(i * step, step)
        place = table.at[1 - h, rows, cols(c)]
        return remote(place, place, fwd_send.at[i], fwd_recv.at[i], b, core_peer)

    core_copy = remote(
        grid_ref, table.at[h, :, cols(c)], core_sem.at[0], core_sem.at[1], b, core_peer
    )
    mesh_copies = [
        remote(mesh_ref, nodes.at[f], mesh_send.at[k - 1], mesh_recv.at[k - 1], b, lax.rem(f + k, nf))
        for k in range(1, nf)
    ]
    core_copy.start()
    x_copies = [x_copy(i) for i in range(CHUNKS)]
    for copy in x_copies:
        copy.start()
    for copy in mesh_copies:
        copy.start()

    nodes[f] = mesh_ref[...]
    table[h, :, cols(c)] = grid_ref[...]

    lane = lax.broadcasted_iota(jnp.int32, (LANES, LANES), 1)

    def build(t, carry):
        if aligned:
            per = quart // LANES
            at = (t // per) * (nf * quart) + f * quart + lax.rem(t, per) * LANES
        else:
            at = t * LANES
        ids = columns(src_ref[:, pl.ds(pl.multiple_of(at, LANES), LANES)])
        rows = pl.ds(pl.multiple_of(t * LANES, LANES), LANES)
        for k in range(grid_rows // LANES):
            hit = jnp.where(lane + k * LANES == ids, 1.0, 0.0)
            onehot[rows, k * LANES : (k + 1) * LANES] = hit.astype(BF16)
        return carry

    lax.fori_loop(0, slots // LANES, build, 0)
    core_copy.wait_recv()

    def band_copy(j, o):
        d = lax.rem(b + o, n)
        return remote(
            outgoing.at[j, o],
            arrived.at[j, b],
            band_send.at[j, o],
            band_recv.at[j, o],
            d,
            f,
        )

    def gather(j, half):
        def piece(o):
            d = lax.rem(b + o, n)
            rows = pl.ds(pl.multiple_of(d * quart, quart), quart)
            return dot(onehot[rows, :], table[half]).astype(BF16)

        def one(o, carry):
            outgoing[j, o] = piece(o)

            @pl.when(o > 1)
            def _():
                band_copy(j, o - 1).start()

            return carry

        lax.fori_loop(1, n, one, 0)
        arrived[j, b] = piece(0)
        band_copy(j, n - 1).start()

    gather(0, h)

    for load in loads[:2]:
        load.wait()
    for copy in mesh_copies:
        copy.wait_recv()
    mesh_wide = jnp.concatenate([nodes[k] for k in range(nf)], axis=1)
    mesh_full[...] = mesh_wide.astype(F32)
    block = 2 * LANES
    node_lane = lax.broadcasted_iota(jnp.int32, (LANES, mesh_rows), 1)
    b1 = b1_ref[...]

    def prepare(t, carry):
        picks = []
        for i in range(2):
            at = pl.multiple_of((2 * t + i) * LANES, LANES)
            ids = columns(dst_wide[:, pl.ds(at, LANES)])
            ids = jnp.minimum(ids, mesh_rows - 1)
            spread = jnp.concatenate([ids] * ((mesh_rows + LANES - 1) // LANES), axis=1)[:, :mesh_rows]
            hit = jnp.where(node_lane == spread, 1.0, 0.0).astype(BF16)
            picks.append(dot(hit, mesh_wide_ref()).astype(BF16))
        receivers = jnp.concatenate(picks, axis=0)
        rows = pl.ds(pl.multiple_of(t * block, block), block)
        base[rows, :] = (
            dot(edge[rows, :], w1[:width, :]) + dot(receivers, w1[2 * width :, :]) + b1
        )
        return carry

    def mesh_wide_ref():
        return jnp.concatenate([nodes[k] for k in range(nf)], axis=1)

    lax.fori_loop(0, slots // block, prepare, 0)
    for load in loads[2:]:
        load.wait()
    my_nodes = pl.ds(pl.multiple_of(f * own_rows, 8), own_rows)
    my_mesh = mesh_full[my_nodes, :]
    node_base = dot(my_mesh.astype(BF16), nw1[:width, :]) + nb1_ref[...]

    fwd_copies = [fwd_copy(i) for i in range(CHUNKS)]
    for i in range(CHUNKS):
        x_copies[i].wait_recv()
        fwd_copies[i].start()
    for copy in fwd_copies:
        copy.wait_recv()
    gather(1, 1 - h)

    b2 = b2_ref[...]
    gain = gain_ref[...]
    shift = shift_ref[...]
    total[...] = jnp.zeros_like(total)
    node_row = lax.broadcasted_iota(jnp.int32, (mesh_rows, quart), 0)

    def edges(o, carry):
        s = lax.rem(b - o + n, n)

        @pl.when(o > 0)
        def _():
            band_copy(0, o).wait_recv()
            band_copy(1, o).wait_recv()

        rows = pl.ds(pl.multiple_of(s * quart, quart), quart)
        low = pl.ds(pl.multiple_of(width + h * pair, pair), pair)
        high = pl.ds(pl.multiple_of(width + (1 - h) * pair, pair), pair)
        hidden = base[rows, :] + dot(arrived[0, s], w1[low, :]) + dot(arrived[1, s], w1[high, :])
        update = dot(silu(hidden).astype(BF16), w2[...]) + b2
        fresh = (edge[rows, :].astype(F32) + normalize(update, gain, shift)).astype(BF16)
        if aligned:
            targets = dst_wide[:, rows]
        else:
            targets = dst_ref[pl.ds(s, 1), :]
        hit = jnp.where(node_row == targets, 1.0, 0.0).astype(BF16)
        total[...] += dot(hit, fresh)
        return carry

    lax.fori_loop(0, n, edges, 0)

    for k in range(nf):
        parts[k] = total[k * own_rows : (k + 1) * own_rows, :].astype(BF16)
    sum_copies = []
    for k in range(1, nf):
        p = lax.rem(f + k, nf)
        sum_copies.append(
            remote(parts.at[p], part_in.at[k - 1], sum_send.at[k - 1], sum_recv.at[k - 1], b, p)
        )
    for copy in sum_copies:
        copy.start()
    summed = parts[f].astype(F32)
    for k in range(1, nf):
        sum_copies[k - 1].wait_recv()
        summed = summed + part_in[k - 1].astype(F32)
    hidden = node_base + dot(summed.astype(BF16), nw1[width:, :])
    update = dot(silu(hidden).astype(BF16), nw2[...]) + nb2_ref[...]
    fresh = (my_mesh + normalize(update, ngain_ref[...], nshift_ref[...])).astype(BF16)
    for k in range(nf):
        cols_out[k] = fresh[:, k * quarter : (k + 1) * quarter]
    out_copies = []
    for k in range(1, nf):
        p = lax.rem(f + k, nf)
        out_copies.append(
            remote(cols_out.at[p], cols_in.at[f], out_send.at[k - 1], out_recv.at[k - 1], b, p)
        )
    for copy in out_copies:
        copy.start()
    cols_in[f] = cols_out[f]
    for copy in out_copies:
        copy.wait_recv()
    out_ref[...] = jnp.concatenate([cols_in[k].astype(F32) for k in range(nf)], axis=0).astype(BF16)

    core_copy.wait_send()
    for copy in x_copies + mesh_copies + fwd_copies + sum_copies + out_copies:
        copy.wait_send()

    def drain(o, carry):
        band_copy(0, o).wait_send()
        band_copy(1, o).wait_send()
        return carry

    lax.fori_loop(1, n, drain, 0)


def body(
    grid_latent,
    mesh_latent,
    edge_latent,
    edge_src,
    edge_dst,
    edge_w1,
    edge_b1,
    edge_w2,
    edge_b2,
    edge_gain,
    edge_shift,
    node_w1,
    node_b1,
    node_w2,
    node_b2,
    node_gain,
    node_shift,
):
    n = lax.axis_size("band")
    nf = lax.axis_size("feat")
    grid_rows, quarter = grid_latent.shape
    width = quarter * nf
    mesh_rows = mesh_latent.shape[0]
    own_rows = mesh_rows // nf
    edges = edge_latent.reshape(-1, width)
    slots = edges.shape[0]
    quart = slots // n
    hidden = edge_w1.shape[1]
    targets = edge_dst.reshape(1, slots)
    if quart % LANES == 0:
        sources, grouped = edge_src, targets
    else:
        sources = lax.dynamic_slice_in_dim(
            edge_src.reshape(n, nf, quart), lax.axis_index("feat"), 1, 1
        ).reshape(1, slots)
        grouped = edge_dst.reshape(n, quart)
    vectors = (edge_b1, edge_b2, edge_gain, edge_shift, node_b1, node_b2, node_gain, node_shift)
    vmem = pl.BlockSpec(memory_space=pltpu.VMEM)
    anyspace = pl.BlockSpec(memory_space=pl.ANY)
    dma = pltpu.SemaphoreType.DMA
    return pl.pallas_call(
        functools.partial(kernel, n, nf),
        out_shape=jax.ShapeDtypeStruct((mesh_rows, quarter), BF16),
        in_specs=[vmem] * 13 + [anyspace] * 5,
        out_specs=vmem,
        scratch_shapes=[
            pltpu.VMEM((slots, width), BF16),
            pltpu.VMEM(edge_w1.shape, BF16),
            pltpu.VMEM(edge_w2.shape, BF16),
            pltpu.VMEM(node_w1.shape, BF16),
            pltpu.VMEM(node_w2.shape, BF16),
            pltpu.VMEM((nf // 2, grid_rows, 2 * quarter), BF16),
            pltpu.VMEM((nf, mesh_rows, quarter), BF16),
            pltpu.VMEM((slots, grid_rows), BF16),
            pltpu.VMEM((2, n, quart, 2 * quarter), BF16),
            pltpu.VMEM((2, n, quart, 2 * quarter), BF16),
            pltpu.VMEM((slots, hidden), F32),
            pltpu.VMEM((mesh_rows, width), F32),
            pltpu.VMEM((mesh_rows, width), F32),
            pltpu.VMEM((nf, own_rows, width), BF16),
            pltpu.VMEM((nf - 1, own_rows, width), BF16),
            pltpu.VMEM((nf, own_rows, quarter), BF16),
            pltpu.VMEM((nf, own_rows, quarter), BF16),
            dma((5,)),
            dma((nf - 1,)),
            dma((nf - 1,)),
            dma((2,)),
            dma((CHUNKS,)),
            dma((CHUNKS,)),
            dma((CHUNKS,)),
            dma((CHUNKS,)),
            dma((2, n)),
            dma((2, n)),
            dma((nf - 1,)),
            dma((nf - 1,)),
            dma((nf - 1,)),
            dma((nf - 1,)),
        ],
        compiler_params=pltpu.CompilerParams(
            collective_id=0, has_side_effects=True, vmem_limit_bytes=56 * 1024 * 1024
        ),
        name="encoder_step",
    )(
        grid_latent,
        mesh_latent,
        sources,
        grouped,
        targets,
        *(v.reshape(1, -1) for v in vectors),
        edges,
        edge_w1,
        edge_w2,
        node_w1,
        node_w2,
    )


def solution(mesh):
    placed = (
        P("band", "feat"),
        P("band", "feat"),
        P("band", "feat", None, None),
        P("band", None),
        P("band", "feat", None),
    ) + (P(),) * 12
    return jax.shard_map(
        body, mesh=mesh, in_specs=placed, out_specs=P("band", "feat"), check_vma=False
    )
```
